256 devices in a mesh: role: 2 (over z_hi), dp: 16 (over y, z_lo), mp: 8 (over x, core).
Axes of the slice: x: 4, y: 4, z: 8 (z_hi: 2, z_lo: 4; z = z_hi * 4 + z_lo), core: 2. Of those that a mesh axis runs over, the one named last changes fastest.
Arguments:
- patches: bfloat16 [25088, 1280], P('dp', 'mp'), may hold values from -6 to 6
- pred_states: bfloat16 [16384, 384], P('dp'), may hold values from -6 to 6
- ema_up: bfloat16 [1280, 5120], P(('role', 'dp'), 'mp'), may hold values from -0.15625 to 0.15625
- ema_down: bfloat16 [5120, 1280], P('mp', ('role', 'dp')), may hold values from -0.078125 to 0.078125
- pred_up: bfloat16 [384, 1536], P(('role', 'dp'), 'mp'), may hold values from -0.3125 to 0.3125
- pred_down: bfloat16 [1536, 384], P('mp', ('role', 'dp')), may hold values from -0.15625 to 0.15625
- pred_out: bfloat16 [384, 1280], P(('role', 'dp'), 'mp'), may hold values from -0.3125 to 0.3125
- masked_index: int32 [16, 1024], P('dp'), may hold values from 0 to 1567, as said below
- masked_count: int32 [16], P('dp'), may hold values from 512 to 1024, as said below
- loss_scale: float32 [], replicated, may hold values from 81920 to 327680
Outputs:
- loss: float32 [], replicated
- grad_up: float32 [384, 1536], P(('role', 'dp'), 'mp')
- grad_down: float32 [1536, 384], P('mp', ('role', 'dp'))
- grad_out: float32 [384, 1280], P(('role', 'dp'), 'mp')
The draws below stay inside these ranges and needn't reach their ends.
Inputs may be any that keep to these rules, and one draw needn't show every extreme that they name: `masked_index`: within a clip the slots name distinct tokens; the slots below masked_count name the masked tokens, which are whole tubes: all 8 frames (token f * 196 + s for frame f) of some spatial positions s. Slots from masked_count on name other tokens and are ignored. `masked_count`: each count is 8 times a whole number; some clip has exactly 1024.
All inputs are finite; a program needn't handle non-finite values.
Results may differ from the reference program's by a relative error of at most 0.012.
Values may be sent and summed in bfloat16 or wider, within the bound.
No kernel may reach another device: no remote copies, remote signals or barrier semaphores. Data moves between devices by JAX's collectives and lax.ppermute only.
A program may use at most 128 MiB of HBM per device.

```python
import math
import jax
import jax.numpy as jnp
from jax import lax

D = 1280
FF = 5120
PW = 384
PF = 1536
FRAMES = 8
SPATIAL = 196
MT = 128
TOK = 1568
MMAX = 1024
CLIPS = 16


def mask_layout(key):
    base = jax.random.fold_in(key, 11)
    clip_keys = jax.random.split(jax.random.fold_in(base, 1), CLIPS)
    spatial_order = jax.vmap(lambda clip_key: jax.random.permutation(clip_key, SPATIAL))(clip_keys).astype(jnp.int32)
    tube_count = jax.random.randint(jax.random.fold_in(base, 2), (CLIPS,), MT // 2, MT + 1)
    fullest = jax.random.randint(jax.random.fold_in(base, 3), (), 0, CLIPS)
    tube_count = jnp.where(jnp.arange(CLIPS) == fullest, MT, tube_count)
    slot_ids = jnp.arange(MMAX, dtype=jnp.int32)
    frame_ids = slot_ids % FRAMES
    spot_ids = spatial_order[:, slot_ids // FRAMES]
    token_ids = (frame_ids * SPATIAL)[None, :] + spot_ids
    return (token_ids.astype(jnp.int32), (tube_count * FRAMES).astype(jnp.int32))


def draw_masked_index(key, part):
    return mask_layout(key)[0]


def draw_masked_count(key, part):
    return mask_layout(key)[1]


def level_of(key, extent, cuts, smallest, largest):
    factor_of = 1.0
    for axis_at, parts in cuts:
        steps = jax.random.uniform(jax.random.fold_in(jax.random.fold_in(key, 6), axis_at), (parts,), jnp.float32, smallest / len(cuts), largest / len(cuts))
        factor_of = factor_of * jnp.repeat(jnp.exp(steps), extent[axis_at] // parts).reshape((-1,) + (1,) * (len(extent) - 1 - axis_at))
    return factor_of


def gaussian(own_key, extent, width, limit, cuts=(), kind=jnp.bfloat16):
    result = width * jax.random.normal(own_key, extent, jnp.float32)
    if cuts:
        result = result * level_of(own_key, extent, cuts, -0.22, 0.18)
    return jnp.clip(result, -limit, limit).astype(kind)


def setup_inputs(seed: int = 0) -> dict:
    splits = jax.random.split(jax.random.key(seed), 11)
    patches = gaussian(splits[0], (CLIPS * TOK, D), 1.0, 6.0, ((0, 16), (1, 8)))
    pred_states = gaussian(splits[1], (CLIPS * MMAX, PW), 1.0, 6.0, ((0, 16),))
    ema_up = gaussian(splits[2], (D, FF), D ** -0.5, 0.15625, ((0, 32), (1, 8)))
    ema_down = gaussian(splits[3], (FF, D), FF ** -0.5, 0.078125, ((0, 8), (1, 32)))
    pred_up = gaussian(splits[4], (PW, PF), PW ** -0.5, 0.3125, ((0, 32), (1, 8)))
    pred_down = gaussian(splits[5], (PF, PW), PF ** -0.5, 0.15625, ((0, 8), (1, 32)))
    pred_out = gaussian(splits[6], (PW, D), PW ** -0.5, 0.3125, ((0, 32), (1, 8)))
    masked_index = draw_masked_index(jax.random.fold_in(splits[10], 71), 0)
    masked_count = draw_masked_count(jax.random.fold_in(splits[10], 71), 0)
    loss_scale = jnp.clip(jnp.exp(jax.random.uniform(splits[9], (), jnp.float32, math.log(81920.0), math.log(327680.0))), 81920.0, 327680.0)
    return {"patches": patches, "pred_states": pred_states, "ema_up": ema_up, "ema_down": ema_down, "pred_up": pred_up, "pred_down": pred_down, "pred_out": pred_out, "masked_index": masked_index, "masked_count": masked_count, "loss_scale": loss_scale}


EPS = 1e-06
COEF = 0.7978845608028654

def normalize(values):
    row_mean = lax.optimization_barrier(jnp.mean(values, axis=-1, keepdims=True))
    row_deviations = values - row_mean
    variance = lax.optimization_barrier(jnp.mean(row_deviations * row_deviations, axis=-1, keepdims=True))
    return row_deviations * lax.rsqrt(variance + EPS)

def gelu_slope(values):
    inner = COEF * (values + 0.044715 * values * values * values)
    tangent = jnp.tanh(inner)
    return 0.5 * (1.0 + tangent) + 0.5 * values * (1.0 - tangent * tangent) * COEF * (1.0 + 3.0 * 0.044715 * values * values)

def reference(patches, pred_states, ema_up, ema_down, pred_up, pred_down, pred_out, masked_index, masked_count, loss_scale):
    clip_count = masked_index.shape[0]

    def target_clip(clip_pair):
        clip_rows, token_index = clip_pair
        normed = normalize(clip_rows.astype(jnp.float32)).astype(jnp.bfloat16)
        hidden = jax.nn.gelu(jnp.dot(normed, ema_up, preferred_element_type=jnp.float32), approximate=True).astype(jnp.bfloat16)
        block_out = clip_rows.astype(jnp.float32) + jnp.dot(hidden, ema_down, preferred_element_type=jnp.float32)
        target_all = normalize(block_out).astype(jnp.bfloat16)
        onehot = (token_index[:, None] == jnp.arange(TOK, dtype=jnp.int32)[None, :]).astype(jnp.bfloat16)
        return jnp.dot(onehot, target_all, preferred_element_type=jnp.float32).astype(jnp.bfloat16)
    targets = lax.map(target_clip, (patches.reshape(clip_count, TOK, D), masked_index))
    targets = targets.reshape(clip_count * MMAX, D)
    states = pred_states.astype(jnp.float32)
    pnormed = normalize(states).astype(jnp.bfloat16)
    preact = jnp.dot(pnormed, pred_up, preferred_element_type=jnp.float32)
    hid_act = jax.nn.gelu(preact, approximate=True).astype(jnp.bfloat16)
    updated = states + jnp.dot(hid_act, pred_down, preferred_element_type=jnp.float32)
    row_mean = lax.optimization_barrier(jnp.mean(updated, axis=-1, keepdims=True))
    row_deviations = updated - row_mean
    reciprocal_spread = lax.rsqrt(lax.optimization_barrier(jnp.mean(row_deviations * row_deviations, axis=-1, keepdims=True)) + EPS)
    standardized_input = row_deviations * reciprocal_spread
    output_normalized = standardized_input.astype(jnp.bfloat16)
    predicted = jnp.dot(output_normalized, pred_out, preferred_element_type=jnp.float32)
    live_mask = (jnp.arange(MMAX, dtype=jnp.int32)[None, :] < masked_count[:, None]).astype(jnp.float32).reshape(clip_count * MMAX, 1)
    total = jnp.sum(masked_count).astype(jnp.float32)
    norm_scale = total * float(D)
    residue = predicted - targets.astype(jnp.float32)
    smooth = jnp.sqrt(residue * residue + 1.0)
    loss = jnp.sum(live_mask * (smooth - 1.0)) / norm_scale
    grad_pred = (loss_scale * live_mask * residue / smooth / norm_scale).astype(jnp.bfloat16)
    grad_out = jnp.dot(output_normalized.T, grad_pred, preferred_element_type=jnp.float32)
    normalized_gradient = jnp.dot(grad_pred, pred_out.T, preferred_element_type=jnp.float32)
    gradient_update = reciprocal_spread * (normalized_gradient - lax.optimization_barrier(jnp.mean(normalized_gradient, axis=-1, keepdims=True)) - standardized_input * lax.optimization_barrier(jnp.mean(normalized_gradient * standardized_input, axis=-1, keepdims=True)))
    gradient_update = gradient_update.astype(jnp.bfloat16)
    grad_down = jnp.dot(hid_act.T, gradient_update, preferred_element_type=jnp.float32)
    grad_act = jnp.dot(gradient_update, pred_down.T, preferred_element_type=jnp.float32)
    grad_pre = (grad_act * gelu_slope(preact)).astype(jnp.bfloat16)
    grad_up = jnp.dot(pnormed.T, grad_pre, preferred_element_type=jnp.float32)
    return (loss, grad_up, grad_down, grad_out)
```

```python
import jax
import jax.numpy as jnp
from jax import lax
from jax.sharding import Mesh
from jax.sharding import PartitionSpec as P

D = 1280
PW = 384
TOK = 1568
MMAX = 1024
X = "mp_0"
CORE = "mp_1"
Y = "dp_0"
Z = ("role", "dp_1")
MP = ("mp_0", "mp_1")
DP = ("dp_0", "dp_1")
ROLE_DP = ("role", "dp_0", "dp_1")

HALF = MMAX // 2
QUARTER = HALF // 2
OWN = QUARTER // 4
EPS = 1e-06
COEF = 0.7978845608028654
BF16 = jnp.bfloat16
F32 = jnp.float32


def spread(block, axis):
    copies = jnp.broadcast_to(block, (lax.axis_size(axis), *block.shape))
    return lax.all_to_all(copies, axis, split_axis=0, concat_axis=0, tiled=True)


def exchanged(pieces, axis):
    return lax.all_to_all(pieces, axis, split_axis=0, concat_axis=0, tiled=True)


def swapped(block):
    return lax.ppermute(block, CORE, [(0, 1), (1, 0)])


def normalize(values, axis=-1):
    row_mean = jnp.mean(values, axis=axis, keepdims=True)
    row_deviations = values - row_mean
    variance = jnp.mean(row_deviations * row_deviations, axis=axis, keepdims=True)
    return row_deviations * lax.rsqrt(variance + EPS)


def gelu_slope(values):
    inner = COEF * (values + 0.044715 * values * values * values)
    tangent = jnp.tanh(inner)
    return 0.5 * (1.0 + tangent) + 0.5 * values * (1.0 - tangent * tangent) * COEF * (
        1.0 + 3.0 * 0.044715 * values * values
    )


def two_parts(value):
    high = lax.reduce_precision(value, 8, 7)
    return jnp.stack([high, lax.reduce_precision(value - high, 8, 7)]).astype(BF16)


def core_major(gathered):
    width = gathered.shape[-1]
    blocks = gathered.reshape(2, 2, 2, 4, -1, width)
    return blocks.transpose(1, 2, 0, 3, 4, 5).reshape(D, width)


def body(
    patches,
    pred_states,
    ema_up,
    ema_down,
    pred_up,
    pred_down,
    pred_out,
    masked_index,
    masked_count,
    loss_scale,
):
    role = lax.axis_index("role")
    core = lax.axis_index(CORE)
    first = core == 0
    start = role * HALF
    own_start = start + core * QUARTER
    other_start = start + (1 - core) * QUARTER
    tile_start = own_start + lax.axis_index(X) * OWN

    both = jnp.concatenate([ema_up, ema_down.T], axis=0)
    along_z = spread(both, Z).reshape(-1, both.shape[1])
    along_y = spread(along_z, Y).reshape(4, 8, 2, 40, both.shape[1])
    up_cols = core_major(along_y[:, :, 0])
    down_rows = core_major(along_y[:, :, 1])

    count = (masked_count[0] // 8).astype(BF16)
    tail = jnp.full((pred_up.shape[0], 96), count, BF16)
    small = jnp.concatenate([pred_up, pred_down.T, pred_out, tail], axis=1)
    small = spread(small, ROLE_DP)
    total = 8.0 * jnp.sum(small[:16, 0, 544].astype(F32))
    small = small.reshape(PW, -1)
    up_rows = small[:, :192]
    down_cols = small[:, 192:384]
    out_x = spread(small[:, 384:544], X)
    out_x = out_x.transpose(1, 0, 2).reshape(PW, D // 2)
    out_other = swapped(out_x)
    out_full = jnp.where(
        first,
        jnp.concatenate([out_x, out_other], axis=1),
        jnp.concatenate([out_other, out_x], axis=1),
    )

    index = jnp.concatenate(
        [
            lax.dynamic_slice_in_dim(masked_index[0], own_start, QUARTER),
            lax.dynamic_slice_in_dim(masked_index[0], other_start, QUARTER),
        ]
    )
    onehot = (jnp.arange(TOK, dtype=jnp.int32)[:, None] == index[None, :]).astype(BF16)
    picked = jnp.einsum("tw,tk->wk", patches, onehot, preferred_element_type=F32).astype(BF16)
    mine = spread(picked, X).reshape(D // 2, HALF)
    theirs = swapped(mine)
    theirs = jnp.concatenate([theirs[:, QUARTER:], theirs[:, :QUARTER]], axis=1)
    whole = jnp.concatenate(
        [jnp.where(first, mine, theirs), jnp.where(first, theirs, mine)], axis=0
    )
    normed = normalize(whole.astype(F32), 0).astype(BF16)
    hidden = jax.nn.gelu(
        jnp.einsum("dr,dh->rh", normed, up_cols, preferred_element_type=F32), approximate=True
    ).astype(BF16)
    for_other = jnp.einsum("rh,dh->rd", hidden[QUARTER:], down_rows, preferred_element_type=F32)
    for_own = jnp.einsum("rh,dh->rd", hidden[:QUARTER], down_rows, preferred_element_type=F32)
    chip_sum = (for_own + swapped(for_other)).astype(BF16)
    arrived = exchanged(chip_sum.reshape(4, OWN, D), X)
    residual = lax.dynamic_slice_in_dim(whole, lax.axis_index(X) * OWN, OWN, 1).T
    block_out = residual.astype(F32) + jnp.sum(arrived.astype(F32), axis=0)
    targets = normalize(block_out).astype(BF16)

    states = jnp.concatenate(
        [
            lax.dynamic_slice_in_dim(pred_states, own_start, QUARTER),
            lax.dynamic_slice_in_dim(pred_states, other_start, QUARTER),
        ]
    ).astype(F32)
    pnormed = normalize(states).astype(BF16)
    preact = jnp.dot(pnormed, up_rows, preferred_element_type=F32)
    hid_act = jax.nn.gelu(preact, approximate=True).astype(BF16)
    mix = jnp.einsum("rf,kf->rk", hid_act, down_cols, preferred_element_type=F32)
    mix = mix[:QUARTER] + swapped(mix[QUARTER:])
    mix = jnp.sum(exchanged(mix.reshape(4, OWN, PW), X), axis=0)
    updated = lax.dynamic_slice_in_dim(pred_states, tile_start, OWN).astype(F32) + mix
    deviations = updated - jnp.mean(updated, axis=-1, keepdims=True)
    reciprocal_spread = lax.rsqrt(jnp.mean(deviations * deviations, axis=-1, keepdims=True) + EPS)
    standardized = deviations * reciprocal_spread
    outnorm = standardized.astype(BF16)
    predicted = jnp.dot(outnorm, out_full, preferred_element_type=F32)
    slots = tile_start + jnp.arange(OWN, dtype=jnp.int32)
    live = (slots < masked_count[0]).astype(F32)[:, None]
    norm_scale = total * float(D)
    residue = predicted - targets.astype(F32)
    smooth = jnp.sqrt(residue * residue + 1.0)
    local_loss = jnp.sum(live * (smooth - 1.0))
    grad_pred = (loss_scale * live * residue / smooth / norm_scale).astype(BF16)
    grad_norm = jnp.einsum("rd,kd->rk", grad_pred, out_full, preferred_element_type=F32)
    grad_upd = reciprocal_spread * (
        grad_norm
        - jnp.mean(grad_norm, axis=-1, keepdims=True)
        - standardized * jnp.mean(grad_norm * standardized, axis=-1, keepdims=True)
    )

    loss_lines = jnp.zeros((16, PW), BF16).at[0, :2].set(two_parts(local_loss))
    lines = jnp.concatenate([grad_upd.astype(BF16), loss_lines], axis=0)
    own_lines = spread(lines, X)
    other_lines = swapped(own_lines)
    rows = jnp.concatenate(
        [own_lines[:, :OWN].reshape(QUARTER, PW), other_lines[:, :OWN].reshape(QUARTER, PW)]
    )
    group_loss = jnp.sum(own_lines[:, OWN, :2].astype(F32)) + jnp.sum(
        other_lines[:, OWN, :2].astype(F32)
    )

    near = jnp.where(first, grad_pred[:, : D // 2], grad_pred[:, D // 2 :])
    far = jnp.where(first, grad_pred[:, D // 2 :], grad_pred[:, : D // 2])
    out_far = jnp.einsum("rk,rd->kd", outnorm, far, preferred_element_type=F32)
    out_near = jnp.einsum("rk,rd->kd", outnorm, near, preferred_element_type=F32)
    out_chip = (out_near + swapped(out_far)).astype(BF16)
    out_local = exchanged(out_chip.reshape(PW, 4, 160).transpose(1, 0, 2), X)
    out_local = jnp.sum(out_local.astype(F32), axis=0).astype(BF16)
    down_local = jnp.einsum("rk,rf->kf", rows, hid_act, preferred_element_type=F32)
    grad_act = jnp.einsum("rk,kf->rf", rows, down_cols, preferred_element_type=F32)
    grad_pre = (grad_act * gelu_slope(preact)).astype(BF16)
    up_local = jnp.einsum("rk,rf->kf", pnormed, grad_pre, preferred_element_type=F32)
    end = jnp.broadcast_to(jnp.pad(two_parts(group_loss), (0, 94)), (PW, 96))
    sent = jnp.concatenate(
        [up_local.astype(BF16), down_local.astype(BF16), out_local, end], axis=1
    )
    sums = exchanged(sent.reshape(32, PW // 32, -1), ROLE_DP)
    sums = jnp.sum(sums.astype(F32), axis=0)
    grad_up = sums[:, :192]
    grad_down = sums[:, 192:384].T
    grad_out = sums[:, 384:544]
    loss = jnp.sum(sums[0, 544:546]) / norm_scale
    return (loss, grad_up, grad_down, grad_out)


def solution(mesh):
    finer = Mesh(
        mesh.devices.reshape(mesh.shape["role"], 4, 4, 4, 2),
        ("role", "dp_0", "dp_1", "mp_0", "mp_1"),
    )
    return jax.shard_map(
        body,
        mesh=finer,
        in_specs=(
            P(DP, MP),
            P(DP, None),
            P(ROLE_DP, MP),
            P(MP, ROLE_DP),
            P(ROLE_DP, MP),
            P(MP, ROLE_DP),
            P(ROLE_DP, MP),
            P(DP, None),
            P(DP),
            P(),
        ),
        out_specs=(P(), P(ROLE_DP, MP), P(MP, ROLE_DP), P(ROLE_DP, MP)),
        check_vma=False,
    )
```
